32 devices in a mesh: section: 8 (over z, core), mp: 4 (over y, x).
Axes of the slice: x: 2, y: 2, z: 4, core: 2. Of those that a mesh axis runs over, the one named last changes fastest.
Arguments:
- arrive_rows: bfloat16 [8, 64, 1024], P('section'), may hold values from -50 to 50
- arrive_grads: bfloat16 [8, 64, 1024], P('section'), may hold values from -6 to 6
- feed_rows: bfloat16 [4, 64, 1024], replicated, may hold values from -50 to 50
- feed_grads: bfloat16 [4, 64, 1024], replicated, may hold values from -6 to 6
- stashed_rows: bfloat16 [8, 5, 64, 1024], P('section'), may hold values from -50 to 50
- slot_order: int32 [8, 5], P('section'), may hold values from 0 to 4, each once within a row
- enter_weight: bfloat16 [8, 1024, 4096], P('section', None, 'mp'), may hold values from -0.1875 to 0.1875
- leave_weight: bfloat16 [8, 4096, 1024], P('section', 'mp'), may hold values from -0.09375 to 0.09375
- norm_gain: bfloat16 [8, 1024], P('section'), may hold values from 0.099609375 to 1.8984375
Outputs:
- depart_rows: bfloat16 [8, 64, 1024], P('section')
- depart_grads: bfloat16 [8, 64, 1024], P('section')
- enter_update: bfloat16 [8, 1024, 4096], P('section', None, 'mp')
- leave_update: bfloat16 [8, 4096, 1024], P('section', 'mp')
- gain_update: float32 [8, 1024], P('section')
The draws below stay inside these ranges and needn't reach their ends.
Inputs may be any that keep to these rules, and one draw needn't show every extreme that they name: `slot_order`: each section's row is a permutation of 0 to 4.
All inputs are finite; a program needn't handle non-finite values.
Results may differ from the reference program's by a relative error of at most 0.025.
Values may be sent and summed in bfloat16 or wider, within the bound.
A program may use at most 128 MiB of HBM per device.

```python
import jax
import jax.numpy as jnp
from jax import lax

D = 1024
HID = 4096
ROWS = 64
STEPS = 5
SECTIONS = 8


def rough_rows(key, shape):
    keys = jax.random.split(key, 3)
    columns = shape[-1]
    ramp = jnp.arange(columns, dtype=jnp.float32) / columns
    column_log = 0.5 * jax.random.uniform(keys[0], (columns,), jnp.float32)
    row_log = jax.random.uniform(keys[1], shape[:-1] + (1,), jnp.float32)
    values = jax.random.normal(keys[2], shape, jnp.float32)
    column_log = column_log + 0.5 * ramp
    values = jnp.clip(values, -5.0, 5.0)
    return values * jnp.power(10.0, column_log + row_log) / 10.0


def draw_arrive_rows(key, part):
    return rough_rows(jax.random.fold_in(key, 31), (SECTIONS, ROWS, D)).astype(jnp.bfloat16)


def draw_feed_rows(key, part):
    return rough_rows(jax.random.fold_in(key, 37), (STEPS - 1, ROWS, D)).astype(jnp.bfloat16)


def draw_stashed_rows(key, part):
    return rough_rows(jax.random.fold_in(key, 41), (SECTIONS, STEPS, ROWS, D)).astype(jnp.bfloat16)


def block_scale(key, extent, cuts, least, high):
    def one(position, shards_of):
        heights = jax.random.uniform(jax.random.fold_in(jax.random.fold_in(key, 6), position), (shards_of,), jnp.float32, least / len(cuts), high / len(cuts))
        return jnp.repeat(jnp.exp(heights), extent[position] // shards_of).reshape((-1,) + (1,) * (len(extent) - position - 1))

    factor_of = one(*cuts[0])
    for cut in cuts[1:]:
        factor_of = factor_of * one(*cut)
    return factor_of


def noise(key, extent, deviation, most, cuts=(), kind=jnp.bfloat16):
    drawn = deviation * jax.random.normal(key, extent, jnp.float32)
    if cuts:
        drawn = drawn * block_scale(key, extent, cuts, -0.22, 0.18)
    return jnp.clip(drawn, -most, most).astype(kind)


def setup_inputs(seed: int = 0) -> dict:
    key_list = jax.random.split(jax.random.key(seed), 10)
    return {
        "arrive_rows": draw_arrive_rows(jax.random.fold_in(key_list[9], 71), 0),
        "arrive_grads": noise(key_list[1], (SECTIONS, ROWS, D), 1.0, 6.0, ((0, 8),)),
        "feed_rows": draw_feed_rows(jax.random.fold_in(key_list[9], 71), 0),
        "feed_grads": noise(key_list[3], (STEPS - 1, ROWS, D), 1.0, 6.0),
        "stashed_rows": draw_stashed_rows(jax.random.fold_in(key_list[9], 71), 0),
        "slot_order": jax.vmap(lambda own: jax.random.permutation(own, STEPS))(jax.random.split(key_list[5], SECTIONS)).reshape((SECTIONS, STEPS)).astype(jnp.int32),
        "enter_weight": noise(key_list[6], (SECTIONS, D, HID), D ** -0.5, 0.1875, ((0, 8), (2, 4))),
        "leave_weight": noise(key_list[7], (SECTIONS, HID, D), HID ** -0.5, 0.09375, ((0, 8), (1, 4))),
        "norm_gain": jnp.clip(1.0 + 0.18 * jax.random.normal(key_list[8], (SECTIONS, D), jnp.float32), 0.099609375, 1.8984375).astype(jnp.bfloat16),
    }


epsilon = 1e-06

def normalize_project(inputs, weight_in, gain_row):
    inputs_wide = inputs.astype(jnp.float32)
    scaled = (inputs_wide * gain_row.astype(jnp.float32)).astype(jnp.bfloat16)
    squares = lax.optimization_barrier(jnp.sum(inputs_wide * inputs_wide, axis=1))
    inverse = lax.rsqrt(squares / D + epsilon)
    projected = jnp.dot(scaled, weight_in, preferred_element_type=jnp.float32)
    return (scaled, inverse, projected)

def section_forward(operands):
    inputs, weight_in, weight_out, gain_row = operands
    scaled, inverse, projected = normalize_project(inputs, weight_in, gain_row)
    hidden = jax.nn.gelu(inverse[:, None] * projected).astype(jnp.bfloat16)
    branch = jnp.dot(hidden, weight_out, preferred_element_type=jnp.float32)
    return (inputs.astype(jnp.float32) + branch).astype(jnp.bfloat16)

def section_backward(operands):
    inputs, output_grad, weight_in, weight_out, gain_row = operands
    scaled, inverse, projected = normalize_project(inputs, weight_in, gain_row)
    preact = inverse[:, None] * projected
    hidden_wide, slope_fn = jax.vjp(jax.nn.gelu, preact)
    hidden = hidden_wide.astype(jnp.bfloat16)
    hidden_grad = jnp.dot(output_grad, weight_out.T, preferred_element_type=jnp.float32)
    pre_grad = slope_fn(hidden_grad)[0]
    scaled_grad = (inverse[:, None] * pre_grad).astype(jnp.bfloat16)
    inverse_grad = lax.optimization_barrier(jnp.sum(pre_grad * projected, axis=1))
    norm_factor = -inverse_grad * inverse * inverse * inverse / D
    input_part = jnp.dot(scaled_grad, weight_in.T, preferred_element_type=jnp.float32)
    inputs_wide = inputs.astype(jnp.float32)
    input_grad = output_grad.astype(jnp.float32) + input_part * gain_row.astype(jnp.float32) + norm_factor[:, None] * inputs_wide
    gain_part = lax.optimization_barrier(jnp.sum(input_part * inputs_wide, axis=0))
    return (input_grad.astype(jnp.bfloat16), hidden, scaled, scaled_grad, gain_part)

def weight_grads(operands):
    hidden_rows, grad_rows, scaled_rows, update_rows = operands
    leave_total = jnp.dot(hidden_rows.T, grad_rows, preferred_element_type=jnp.float32)
    enter_total = jnp.dot(scaled_rows.T, update_rows, preferred_element_type=jnp.float32)
    return (enter_total.astype(jnp.bfloat16), leave_total.astype(jnp.bfloat16))

def reference(arrive_rows, arrive_grads, feed_rows, feed_grads, stashed_rows, slot_order, enter_weight, leave_weight, norm_gain):
    section_count = arrive_rows.shape[0]
    section_ids = jnp.arange(section_count, dtype=jnp.int32)
    inputs_now = arrive_rows
    grads_now = arrive_grads
    gain_total = jnp.zeros(norm_gain.shape, jnp.float32)
    hidden_steps = []
    grad_steps = []
    scaled_steps = []
    update_steps = []
    outputs = arrive_rows
    input_grad = arrive_grads
    for step in range(STEPS):
        outputs = lax.map(section_forward, (inputs_now, enter_weight, leave_weight, norm_gain))
        picked = stashed_rows[section_ids, slot_order[:, step].astype(jnp.int32)]
        input_grad, hidden, scaled, scaled_grad, gain_part = lax.map(section_backward, (picked, grads_now, enter_weight, leave_weight, norm_gain))
        hidden_steps.append(hidden)
        grad_steps.append(grads_now)
        scaled_steps.append(scaled)
        update_steps.append(scaled_grad)
        gain_total = gain_total + gain_part
        if step + 1 < STEPS:
            inputs_now = jnp.concatenate([feed_rows[step][None], outputs[:-1]], axis=0)
            grads_now = jnp.concatenate([input_grad[1:], feed_grads[step][None]], axis=0)
    stacked = (jnp.concatenate(hidden_steps, axis=1), jnp.concatenate(grad_steps, axis=1), jnp.concatenate(scaled_steps, axis=1), jnp.concatenate(update_steps, axis=1))
    enter_update, leave_update = lax.map(weight_grads, stacked)
    return (outputs, input_grad, enter_update, leave_update, gain_total)
```

```python
import functools

import jax
import jax.numpy as jnp
from jax import lax
from jax.experimental import pallas as pl
from jax.experimental.pallas import tpu as pltpu
from jax.sharding import PartitionSpec as P

MESH = pl.DeviceIdType.MESH
F32 = jnp.float32
BF16 = jnp.bfloat16
epsilon = 1e-06
ROOT = 0.7978845608028654
CUBE = 0.044715


def dot(left, right, over_left, over_right):
    return lax.dot_general(
        left, right, (((over_left,), (over_right,)), ((), ())), preferred_element_type=F32
    )


def kernel(
    sections,
    peers,
    slot_ref,
    arrive_rows,
    arrive_grads,
    feed_rows,
    feed_grads,
    stashed,
    win,
    wout,
    gain,
    depart_rows,
    depart_grads,
    enter_out,
    leave_out,
    gain_out,
    rows_in,
    grads_in,
    part_send,
    part_recv,
    sum_send,
    own_rows,
    own_grads,
    slot_rows,
    slot_scaled,
    slot_hidden,
    slot_proj,
    slot_slope,
    slot_inverse,
    slot_update,
    grads_all,
    gain_acc,
    gain_send,
    gain_recv,
    part_ssem,
    part_rsem,
    sum_ssem,
    sum_rsem,
    gain_ssem,
    gain_rsem,
):
    sec = lax.axis_index("section")
    me = lax.axis_index("mp")
    steps, rows, width = stashed.shape
    hidden_width = win.shape[1]
    block = width // peers
    not_first = sec > 0
    not_last = sec < sections - 1

    def ahead(k):
        return lax.rem(me + k, peers)

    def behind(k):
        return lax.rem(me + peers - k, peers)

    def span(p):
        return pl.ds(pl.multiple_of(p * block, block), block)

    barrier = pltpu.get_barrier_semaphore()

    def greet(section, p):
        pl.semaphore_signal(barrier, inc=1, device_id=(section, p), device_id_type=MESH)

    for k in range(1, peers):
        greet(sec, ahead(k))

    @pl.when(not_first)
    def _():
        for k in range(peers):
            greet(sec - 1, ahead(k))

    @pl.when(not_last)
    def _():
        for k in range(peers):
            greet(sec + 1, ahead(k))

    expected = (
        peers - 1
        + peers * jnp.where(not_first, 1, 0)
        + peers * jnp.where(not_last, 1, 0)
    )

    for p in range(peers):
        cut = pl.ds(p * block, block)
        rows_in[0, p] = arrive_rows[:, cut]
        grads_in[0, p] = arrive_grads[:, cut]

    @pl.when(sec == 0)
    def _():
        for t in range(1, steps):
            for p in range(peers):
                rows_in[t, p] = feed_rows[t - 1, :, pl.ds(p * block, block)]

    @pl.when(sec == sections - 1)
    def _():
        for t in range(1, steps):
            for p in range(peers):
                grads_in[t, p] = feed_grads[t - 1, :, pl.ds(p * block, block)]

    gain_acc[...] = jnp.zeros_like(gain_acc)

    def part_copy(way, t, k):
        return pltpu.make_async_remote_copy(
            src_ref=part_send.at[way, t, k - 1],
            dst_ref=part_recv.at[way, t, k - 1],
            send_sem=part_ssem.at[way, t, k - 1],
            recv_sem=part_rsem.at[way, t, k - 1],
            device_id=(sec, ahead(k)),
            device_id_type=MESH,
        )

    def sum_copy(way, t, k, section, p):
        land = (rows_in, grads_in)[way]
        return pltpu.make_async_remote_copy(
            src_ref=sum_send.at[way, t],
            dst_ref=land.at[t + 1, me],
            send_sem=sum_ssem.at[way, t, k],
            recv_sem=sum_rsem.at[way, t, k],
            device_id=(section, p),
            device_id_type=MESH,
        )

    def sum_wait(way, t, k):
        land = (rows_in, grads_in)[way]
        pltpu.make_async_remote_copy(
            src_ref=sum_send.at[way, t],
            dst_ref=land.at[t + 1, behind(k)],
            send_sem=sum_ssem.at[way, t, k],
            recv_sem=sum_rsem.at[way, t, k],
            device_id=(sec, behind(k)),
            device_id_type=MESH,
        ).wait_recv()

    def forward(t):
        total = jnp.zeros((rows, hidden_width), F32)
        squares = jnp.zeros((rows, 1), F32)
        for k in range(peers):
            p = behind(k)

            @pl.when((t > 0) & not_first)
            def _():
                sum_wait(0, t - 1, k)

            wide = rows_in[t, p].astype(F32)
            scaled = (wide * gain[:, span(p)]).astype(BF16)
            total = total + dot(scaled, win[span(p), :], 1, 0)
            squares = squares + jnp.sum(wide * wide, axis=1, keepdims=True)
        z = lax.rsqrt(squares / width + epsilon) * total
        half = 0.5 * z
        hidden = (half + half * jnp.tanh(ROOT * (z + CUBE * (z * z * z)))).astype(BF16)

        @pl.when(t == 0)
        def _():
            pl.semaphore_wait(barrier, expected)

        for k in list(range(1, peers)) + [0]:
            part = dot(hidden, wout[:, span(ahead(k))], 1, 0)
            if k:
                part_send[0, t, k - 1] = part.astype(BF16)
                part_copy(0, t, k).start()
            else:
                own_rows[...] = part + rows_in[t, me].astype(F32)

    def prepare():
        for t in range(steps):
            slot = stashed[slot_ref[0, t]]
            slot_rows[t] = slot
            wide = slot.astype(F32)
            slot_scaled[t] = (wide * gain[...]).astype(BF16)
            slot_inverse[t] = lax.rsqrt(
                jnp.sum(wide * wide, axis=1, keepdims=True) / width + epsilon
            )
        flat = slot_scaled[...].reshape(steps * rows, width)
        slot_proj[...] = dot(flat, win[...], 1, 0).reshape(steps, rows, hidden_width)

        def shape_slot(t, carry):
            z = slot_inverse[t] * slot_proj[t]
            inner = ROOT * (z + CUBE * (z * z * z))
            bend = jnp.tanh(inner)
            half = 0.5 * z
            slot_hidden[t] = (half + half * bend).astype(BF16)
            slot_slope[t] = 0.5 * (1.0 + bend) + half * (1.0 - bend * bend) * (
                ROOT * (1.0 + (3.0 * CUBE) * (z * z))
            )
            return carry

        lax.fori_loop(0, steps, shape_slot, 0)

    def backward(t):
        total = jnp.zeros((rows, hidden_width), F32)
        for k in range(peers):
            p = behind(k)

            @pl.when((t > 0) & not_last)
            def _():
                sum_wait(1, t - 1, k)

            piece = grads_in[t, p]
            grads_all[t, :, span(p)] = piece
            total = total + dot(piece, wout[:, span(p)], 1, 1)
        pre_grad = total * slot_slope[t]
        inverse = slot_inverse[t]
        update = (inverse * pre_grad).astype(BF16)
        slot_update[t] = update
        dots = jnp.sum(pre_grad * slot_proj[t], axis=1, keepdims=True)
        factor = -dots * (inverse * inverse * inverse) / width
        for k in list(range(1, peers)) + [0]:
            p = ahead(k)
            raw = dot(update, win[span(p), :], 1, 1)
            wide = slot_rows[t, :, span(p)].astype(F32)
            gain_acc[p] += jnp.sum((raw * wide).reshape(rows // 8, 8, block), axis=0)
            part = raw * gain[:, span(p)] + factor * wide
            if k:
                part_send[1, t, k - 1] = part.astype(BF16)
                part_copy(1, t, k).start()
            else:
                own_grads[...] = part + grads_in[t, me].astype(F32)

    def reduce(way, t):
        own = (own_rows, own_grads)[way]
        land = (rows_in, grads_in)[way]
        total = own[...]
        for k in range(1, peers):
            part_copy(way, t, k).wait_recv()
            total = total + part_recv[way, t, k - 1].astype(F32)
        sum_send[way, t] = total.astype(BF16)

        @pl.when((t < steps - 1) & (not_last if way == 0 else not_first))
        def _():
            for k in range(peers):
                sum_copy(way, t, k, sec + 1 if way == 0 else sec - 1, ahead(k)).start()

        @pl.when(t == steps - 1)
        def _():
            land[steps, me] = total.astype(BF16)
            for k in range(1, peers):
                sum_copy(way, t, k, sec, ahead(k)).start()

    def gain_copy(k):
        return pltpu.make_async_remote_copy(
            src_ref=gain_send,
            dst_ref=gain_recv.at[k - 1],
            send_sem=gain_ssem.at[k - 1],
            recv_sem=gain_rsem.at[k - 1],
            device_id=(sec, ahead(k)),
            device_id_type=MESH,
        )

    chunk = min(256, hidden_width)

    def leave_grad():
        right = grads_all[...].reshape(steps * rows, width)

        def go(i, carry):
            cut = pl.ds(pl.multiple_of(i * chunk, chunk), chunk)
            left = slot_hidden[:, :, cut].reshape(steps * rows, chunk)
            leave_out[cut, :] = dot(left, right, 0, 0).astype(BF16)
            return carry

        lax.fori_loop(0, hidden_width // chunk, go, 0)

    def enter_grad():
        right = slot_update[...].reshape(steps * rows, hidden_width)
        deep = min(256, width)

        def go(i, carry):
            cut = pl.ds(pl.multiple_of(i * deep, deep), deep)
            left = slot_scaled[:, :, cut].reshape(steps * rows, deep)
            enter_out[cut, :] = dot(left, right, 0, 0).astype(BF16)
            return carry

        lax.fori_loop(0, width // deep, go, 0)

    def step(t, carry):
        forward(t)

        @pl.when(t == 0)
        def _():
            prepare()

        backward(t)

        @pl.when(t == steps - 1)
        def _():
            for p in range(peers):
                gain_send[pl.ds(p, 1), :] = jnp.sum(gain_acc[p], axis=0, keepdims=True)
            for k in range(1, peers):
                gain_copy(k).start()

        reduce(0, t)

        @pl.when(t == steps - 1)
        def _():
            leave_grad()

        reduce(1, t)
        return carry

    lax.fori_loop(0, steps, step, 0)
    enter_grad()

    gains = gain_send[...]
    for k in range(1, peers):
        gain_copy(k).wait_recv()
        gains = gains + gain_recv[k - 1]
    for p in range(peers):
        gain_out[:, pl.ds(p * block, block)] = gains[p : p + 1, :]

    for way, out in ((0, depart_rows), (1, depart_grads)):
        land = (rows_in, grads_in)[way]
        for k in range(1, peers):
            sum_wait(way, steps - 1, k)
        for p in range(peers):
            out[:, pl.ds(p * block, block)] = land[steps, p]

    for k in range(1, peers):
        gain_copy(k).wait_send()

    def drain(t, carry):
        for way in (0, 1):
            for k in range(1, peers):
                part_copy(way, t, k).wait_send()
            for k in range(peers):
                sends = not_last if way == 0 else not_first
                final = t == steps - 1
                sends = (sends & (t < steps - 1)) | final if k else sends & (t < steps - 1)

                @pl.when(sends)
                def _():
                    sum_copy(way, t, k, sec, me).wait_send()

        return carry

    lax.fori_loop(0, steps, drain, 0)


def solution(mesh):
    sections = mesh.shape["section"]
    peers = mesh.shape["mp"]

    def local(
        arrive_rows,
        arrive_grads,
        feed_rows,
        feed_grads,
        stashed_rows,
        slot_order,
        enter_weight,
        leave_weight,
        norm_gain,
    ):
        _, steps, rows, width = stashed_rows.shape
        hidden_width = enter_weight.shape[2]
        block = width // peers
        vmem = pl.BlockSpec(memory_space=pltpu.VMEM)
        dma = pltpu.SemaphoreType.DMA
        outs = pl.pallas_call(
            functools.partial(kernel, sections, peers),
            out_shape=(
                jax.ShapeDtypeStruct((rows, width), BF16),
                jax.ShapeDtypeStruct((rows, width), BF16),
                jax.ShapeDtypeStruct((width, hidden_width), BF16),
                jax.ShapeDtypeStruct((hidden_width, width), BF16),
                jax.ShapeDtypeStruct((1, width), F32),
            ),
            in_specs=[pl.BlockSpec(memory_space=pltpu.SMEM)] + [vmem] * 8,
            out_specs=[vmem] * 5,
            scratch_shapes=[
                pltpu.VMEM((steps + 1, peers, rows, block), BF16),
                pltpu.VMEM((steps + 1, peers, rows, block), BF16),
                pltpu.VMEM((2, steps, peers - 1, rows, block), BF16),
                pltpu.VMEM((2, steps, peers - 1, rows, block), BF16),
                pltpu.VMEM((2, steps, rows, block), BF16),
                pltpu.VMEM((rows, block), F32),
                pltpu.VMEM((rows, block), F32),
                pltpu.VMEM((steps, rows, width), BF16),
                pltpu.VMEM((steps, rows, width), BF16),
                pltpu.VMEM((steps, rows, hidden_width), BF16),
                pltpu.VMEM((steps, rows, hidden_width), F32),
                pltpu.VMEM((steps, rows, hidden_width), F32),
                pltpu.VMEM((steps, rows, 1), F32),
                pltpu.VMEM((steps, rows, hidden_width), BF16),
                pltpu.VMEM((steps, rows, width), BF16),
                pltpu.VMEM((peers, 8, block), F32),
                pltpu.VMEM((peers, block), F32),
                pltpu.VMEM((peers - 1, peers, block), F32),
                dma((2, steps, peers - 1)),
                dma((2, steps, peers - 1)),
                dma((2, steps, peers)),
                dma((2, steps, peers)),
                dma((peers - 1,)),
                dma((peers - 1,)),
            ],
            compiler_params=pltpu.CompilerParams(
                collective_id=0, has_side_effects=True, vmem_limit_bytes=56 * 1024 * 1024
            ),
        )(
            slot_order,
            arrive_rows[0],
            arrive_grads[0],
            feed_rows,
            feed_grads,
            stashed_rows[0],
            enter_weight[0],
            leave_weight[0],
            norm_gain.astype(F32),
        )
        rows_out, grads_out, enter_total, leave_total, gain_total = outs
        return (
            rows_out[None],
            grads_out[None],
            enter_total[None],
            leave_total[None],
            gain_total,
        )

    return jax.shard_map(
        local,
        mesh=mesh,
        in_specs=(
            P("section", None, None),
            P("section", None, None),
            P(),
            P(),
            P("section", None, None, None),
            P("section", None),
            P("section", None, "mp"),
            P("section", "mp", None),
            P("section", None),
        ),
        out_specs=(
            P("section", None, None),
            P("section", None, None),
            P("section", None, "mp"),
            P("section", "mp", None),
            P("section", None),
        ),
        check_vma=False,
    )
```

```python
import functools

import jax
import jax.numpy as jnp
from jax import lax
from jax.experimental import pallas as pl
from jax.experimental.pallas import tpu as pltpu
from jax.sharding import PartitionSpec as P

MESH = pl.DeviceIdType.MESH
F32 = jnp.float32
BF16 = jnp.bfloat16
epsilon = 1e-06
ROOT = 0.7978845608028654
CUBE = 0.044715


def dot(left, right, over_left, over_right):
    return lax.dot_general(
        left, right, (((over_left,), (over_right,)), ((), ())), preferred_element_type=F32
    )


def kernel(
    sections,
    peers,
    slot_hbm,
    arrive_rows,
    arrive_grads,
    feed_rows,
    feed_grads,
    stash_hbm,
    win_hbm,
    wout_hbm,
    gain_hbm,
    depart_rows,
    depart_grads,
    enter_out,
    leave_out,
    gain_out,
    stashed,
    win,
    wout,
    gain,
    rows_in,
    grads_in,
    part_send,
    part_recv,
    sum_send,
    own_rows,
    own_grads,
    slot_rows,
    slot_scaled,
    slot_hidden,
    slot_proj,
    slot_slope,
    slot_inverse,
    slot_update,
    grads_all,
    gain_acc,
    gain_send,
    gain_recv,
    part_ssem,
    part_rsem,
    sum_ssem,
    sum_rsem,
    gain_ssem,
    gain_rsem,
    load_sem,
    feed_sem,
    slot_ref,
    gain_row,
):
    sec = lax.axis_index("section")
    me = lax.axis_index("mp")
    steps, rows, width = stashed.shape
    hidden_width = win.shape[1]
    block = width // peers
    not_first = sec > 0
    not_last = sec < sections - 1

    pairs = (me, 3 - me, lax.rem(5 - me, 4), lax.rem(me + 2, 4)) if peers == 4 else None

    def ahead(k):
        return lax.rem(me + k, peers) if pairs is None else pairs[k]

    def behind(k):
        return lax.rem(me + peers - k, peers) if pairs is None else pairs[k]

    order = list(range(1, peers)) + [0]
    loads = [
        pltpu.make_async_copy(source, target, load_sem.at[i])
        for i, (source, target) in enumerate(
            ((win_hbm, win), (wout_hbm, wout), (stash_hbm, stashed), (gain_hbm, gain_row), (slot_hbm, slot_ref))
        )
    ]

    def load(way, t, p):
        cut = span(p)
        if isinstance(t, int) and t == 0:
            source = (arrive_rows, arrive_grads)[way].at[:, cut]
        else:
            source = (feed_rows, feed_grads)[way].at[t - 1, :, cut]
        return pltpu.make_async_copy(
            source, (rows_in, grads_in)[way].at[t, p], feed_sem.at[way, t, p]
        )

    def span(p):
        return pl.ds(pl.multiple_of(p * block, block), block)

    for p in range(peers):
        load(0, 0, p).start()
    for i in (3, 0, 1, 2, 4):
        loads[i].start()
    for p in range(peers):
        load(1, 0, p).start()

    @pl.when(sec == 0)
    def _():
        for t in range(1, steps):
            for p in range(peers):
                load(0, t, p).start()

    @pl.when(sec == sections - 1)
    def _():
        for t in range(1, steps):
            for p in range(peers):
                load(1, t, p).start()

    barrier = pltpu.get_barrier_semaphore()

    def greet(section, p):
        pl.semaphore_signal(barrier, inc=1, device_id=(section, p), device_id_type=MESH)

    for k in range(1, peers):
        greet(sec, ahead(k))

    @pl.when(not_first)
    def _():
        for k in range(peers):
            greet(sec - 1, ahead(k))

    @pl.when(not_last)
    def _():
        for k in range(peers):
            greet(sec + 1, ahead(k))

    expected = (
        peers - 1
        + peers * jnp.where(not_first, 1, 0)
        + peers * jnp.where(not_last, 1, 0)
    )

    gain_acc[...] = jnp.zeros_like(gain_acc)

    def part_copy(way, t, k):
        return pltpu.make_async_remote_copy(
            src_ref=part_send.at[way, t, k - 1],
            dst_ref=part_recv.at[way, t, k - 1],
            send_sem=part_ssem.at[way, t, k - 1],
            recv_sem=part_rsem.at[way, t, k - 1],
            device_id=(sec, ahead(k)),
            device_id_type=MESH,
        )

    def sum_copy(way, t, k, section, p):
        land = (rows_in, grads_in)[way]
        return pltpu.make_async_remote_copy(
            src_ref=sum_send.at[way, t],
            dst_ref=land.at[t + 1, me],
            send_sem=sum_ssem.at[way, t, k],
            recv_sem=sum_rsem.at[way, t, k],
            device_id=(section, p),
            device_id_type=MESH,
        )

    def sum_wait(way, t, k):
        land = (rows_in, grads_in)[way]
        pltpu.make_async_remote_copy(
            src_ref=sum_send.at[way, t],
            dst_ref=land.at[t + 1, behind(k)],
            send_sem=sum_ssem.at[way, t, k],
            recv_sem=sum_rsem.at[way, t, k],
            device_id=(sec, behind(k)),
            device_id_type=MESH,
        ).wait_recv()

    def arrived(way, t, k, travels):
        @pl.when(t == 0)
        def _():
            load(way, 0, behind(k)).wait()

        @pl.when((t > 0) & jnp.logical_not(travels))
        def _():
            load(way, t, behind(k)).wait()

        @pl.when((t > 0) & travels)
        def _():
            sum_wait(way, t - 1, k)

    def forward(t):
        total = jnp.zeros((rows, hidden_width), F32)
        squares = jnp.zeros((rows, 1), F32)
        for k in range(peers):
            p = behind(k)

            arrived(0, t, k, not_first)

            wide = rows_in[t, p].astype(F32)
            scaled = (wide * gain[:, span(p)]).astype(BF16)
            total = total + dot(scaled, win[span(p), :], 1, 0)
            squares = squares + jnp.sum(wide * wide, axis=1, keepdims=True)
        z = lax.rsqrt(squares / width + epsilon) * total
        half = 0.5 * z
        hidden = (half + half * jnp.tanh(ROOT * (z + CUBE * (z * z * z)))).astype(BF16)

        @pl.when(t == 0)
        def _():
            pl.semaphore_wait(barrier, expected)
            loads[1].wait()

        for k in order:
            part = dot(hidden, wout[:, span(ahead(k))], 1, 0)
            if k:
                part_send[0, t, k - 1] = part.astype(BF16)
                part_copy(0, t, k).start()
            else:
                own_rows[...] = part + rows_in[t, me].astype(F32)

    def prepare(t):
        slot = stashed[slot_ref[0, t]]
        slot_rows[t] = slot
        wide = slot.astype(F32)
        scaled = (wide * gain[...]).astype(BF16)
        slot_scaled[t] = scaled
        inverse = lax.rsqrt(jnp.sum(wide * wide, axis=1, keepdims=True) / width + epsilon)
        slot_inverse[...] = inverse
        projected = dot(scaled, win[...], 1, 0)
        slot_proj[...] = projected
        z = inverse * projected
        bend = jnp.tanh(ROOT * (z + CUBE * (z * z * z)))
        half = 0.5 * z
        slot_hidden[t] = (half + half * bend).astype(BF16)
        slot_slope[...] = 0.5 * (1.0 + bend) + half * (1.0 - bend * bend) * (
            ROOT * (1.0 + (3.0 * CUBE) * (z * z))
        )

    def backward(t):
        total = jnp.zeros((rows, hidden_width), F32)
        for k in range(peers):
            p = behind(k)

            arrived(1, t, k, not_last)

            piece = grads_in[t, p]
            grads_all[t, :, span(p)] = piece
            total = total + dot(piece, wout[:, span(p)], 1, 1)
        pre_grad = total * slot_slope[...]
        inverse = slot_inverse[...]
        update = (inverse * pre_grad).astype(BF16)
        slot_update[t] = update
        dots = jnp.sum(pre_grad * slot_proj[...], axis=1, keepdims=True)
        factor = -dots * (inverse * inverse * inverse) / width
        for k in order:
            p = ahead(k)
            raw = dot(update, win[span(p), :], 1, 1)
            wide = slot_rows[t, :, span(p)].astype(F32)
            gain_acc[p] += jnp.sum((raw * wide).reshape(rows // 8, 8, block), axis=0)
            part = raw * gain[:, span(p)] + factor * wide
            if k:
                part_send[1, t, k - 1] = part.astype(BF16)
                part_copy(1, t, k).start()
            else:
                own_grads[...] = part + grads_in[t, me].astype(F32)

    def reduce(way, t):
        own = (own_rows, own_grads)[way]
        land = (rows_in, grads_in)[way]
        total = own[...]
        for k in range(1, peers):
            part_copy(way, t, k).wait_recv()
            total = total + part_recv[way, t, k - 1].astype(F32)
        sum_send[way, t] = total.astype(BF16)

        @pl.when((t < steps - 1) & (not_last if way == 0 else not_first))
        def _():
            for k in order:
                sum_copy(way, t, k, sec + 1 if way == 0 else sec - 1, ahead(k)).start()

        @pl.when(t == steps - 1)
        def _():
            land[steps, me] = total.astype(BF16)
            for k in range(1, peers):
                sum_copy(way, t, k, sec, ahead(k)).start()

    def gain_copy(k):
        return pltpu.make_async_remote_copy(
            src_ref=gain_send,
            dst_ref=gain_recv.at[k - 1],
            send_sem=gain_ssem.at[k - 1],
            recv_sem=gain_rsem.at[k - 1],
            device_id=(sec, ahead(k)),
            device_id_type=MESH,
        )

    chunk = min(256, hidden_width)

    def leave_grad():
        right = grads_all[...].reshape(steps * rows, width)

        def go(i, carry):
            cut = pl.ds(pl.multiple_of(i * chunk, chunk), chunk)
            left = slot_hidden[:, :, cut].reshape(steps * rows, chunk)
            leave_out[cut, :] = dot(left, right, 0, 0).astype(BF16)
            return carry

        lax.fori_loop(0, hidden_width // chunk, go, 0)

    def enter_grad():
        right = slot_update[...].reshape(steps * rows, hidden_width)
        deep = min(256, width)

        def go(i, carry):
            cut = pl.ds(pl.multiple_of(i * deep, deep), deep)
            left = slot_scaled[:, :, cut].reshape(steps * rows, deep)
            enter_out[cut, :] = dot(left, right, 0, 0).astype(BF16)
            return carry

        lax.fori_loop(0, width // deep, go, 0)

    def step(t, carry):
        forward(t)

        @pl.when(t == 0)
        def _():
            loads[2].wait()
            loads[4].wait()

        prepare(t)

        backward(t)

        @pl.when(t == steps - 1)
        def _():
            for p in range(peers):
                gain_send[pl.ds(p, 1), :] = jnp.sum(gain_acc[p], axis=0, keepdims=True)
            for k in range(1, peers):
                gain_copy(k).start()

        reduce(0, t)

        @pl.when(t == steps - 1)
        def _():
            leave_grad()

        reduce(1, t)
        return carry

    loads[3].wait()
    gain[...] = gain_row[...].astype(F32)
    loads[0].wait()
    lax.fori_loop(0, steps, step, 0)
    enter_grad()

    gains = gain_send[...]
    for k in range(1, peers):
        gain_copy(k).wait_recv()
        gains = gains + gain_recv[k - 1]
    for p in range(peers):
        gain_out[:, pl.ds(p * block, block)] = gains[p : p + 1, :]

    for way, out in ((0, depart_rows), (1, depart_grads)):
        land = (rows_in, grads_in)[way]
        for k in range(1, peers):
            sum_wait(way, steps - 1, k)
        for p in range(peers):
            out[:, pl.ds(p * block, block)] = land[steps, p]

    for k in range(1, peers):
        gain_copy(k).wait_send()

    def drain(t, carry):
        for way in (0, 1):
            for k in range(1, peers):
                part_copy(way, t, k).wait_send()
            for k in range(peers):
                sends = not_last if way == 0 else not_first
                final = t == steps - 1
                sends = (sends & (t < steps - 1)) | final if k else sends & (t < steps - 1)

                @pl.when(sends)
                def _():
                    sum_copy(way, t, k, sec, me).wait_send()

        return carry

    lax.fori_loop(0, steps, drain, 0)


def flush(*refs):
    sems = refs[10]
    copies = [pltpu.make_async_copy(refs[i], refs[i + 5], sems.at[i]) for i in range(5)]
    for copy in copies:
        copy.start()
    for copy in copies:
        copy.wait()


def solution(mesh):
    sections = mesh.shape["section"]
    peers = mesh.shape["mp"]

    def local(
        arrive_rows,
        arrive_grads,
        feed_rows,
        feed_grads,
        stashed_rows,
        slot_order,
        enter_weight,
        leave_weight,
        norm_gain,
    ):
        _, steps, rows, width = stashed_rows.shape
        hidden_width = enter_weight.shape[2]
        block = width // peers
        vmem = pl.BlockSpec(memory_space=pltpu.VMEM)
        hbm = pl.BlockSpec(memory_space=pltpu.HBM)
        dma = pltpu.SemaphoreType.DMA
        kinds = (
            ((rows, width), BF16),
            ((rows, width), BF16),
            ((width, hidden_width), BF16),
            ((hidden_width, width), BF16),
            ((1, width), F32),
        )
        outs = pl.pallas_call(
            functools.partial(kernel, sections, peers),
            out_shape=tuple(pltpu.VMEM(shape, kind) for shape, kind in kinds),
            in_specs=[hbm] * 9,
            out_specs=[vmem] * 5,
            scratch_shapes=[
                pltpu.VMEM((steps, rows, width), BF16),
                pltpu.VMEM((width, hidden_width), BF16),
                pltpu.VMEM((hidden_width, width), BF16),
                pltpu.VMEM((1, width), F32),
                pltpu.VMEM((steps + 1, peers, rows, block), BF16),
                pltpu.VMEM((steps + 1, peers, rows, block), BF16),
                pltpu.VMEM((2, steps, peers - 1, rows, block), BF16),
                pltpu.VMEM((2, steps, peers - 1, rows, block), BF16),
                pltpu.VMEM((2, steps, rows, block), BF16),
                pltpu.VMEM((rows, block), F32),
                pltpu.VMEM((rows, block), F32),
                pltpu.VMEM((steps, rows, width), BF16),
                pltpu.VMEM((steps, rows, width), BF16),
                pltpu.VMEM((steps, rows, hidden_width), BF16),
                pltpu.VMEM((rows, hidden_width), F32),
                pltpu.VMEM((rows, hidden_width), F32),
                pltpu.VMEM((rows, 1), F32),
                pltpu.VMEM((steps, rows, hidden_width), BF16),
                pltpu.VMEM((steps, rows, width), BF16),
                pltpu.VMEM((peers, 8, block), F32),
                pltpu.VMEM((peers, block), F32),
                pltpu.VMEM((peers - 1, peers, block), F32),
                dma((2, steps, peers - 1)),
                dma((2, steps, peers - 1)),
                dma((2, steps, peers)),
                dma((2, steps, peers)),
                dma((peers - 1,)),
                dma((peers - 1,)),
                dma((5,)),
                dma((2, steps, peers)),
                pltpu.SMEM((1, steps), jnp.int32),
                pltpu.VMEM((1, width), BF16),
            ],
            compiler_params=pltpu.CompilerParams(
                collective_id=0, has_side_effects=True, vmem_limit_bytes=40_000_000
            ),
        )(
            *[
                pltpu.with_memory_space_constraint(block_in, pltpu.HBM)
                for block_in in (
                    slot_order,
                    arrive_rows[0],
                    arrive_grads[0],
                    feed_rows,
                    feed_grads,
                    stashed_rows[0],
                    enter_weight[0],
                    leave_weight[0],
                    norm_gain,
                )
            ],
        )
        outs = pl.pallas_call(
            flush,
            out_shape=tuple(jax.ShapeDtypeStruct(shape, kind) for shape, kind in kinds),
            in_specs=[pl.BlockSpec(memory_space=pl.ANY)] * 5,
            out_specs=[hbm] * 5,
            scratch_shapes=[dma((5,))],
            compiler_params=pltpu.CompilerParams(vmem_limit_bytes=1024 * 1024),
        )(*[pltpu.with_memory_space_constraint(out, pltpu.VMEM) for out in outs])
        rows_out, grads_out, enter_total, leave_total, gain_total = outs
        return (
            rows_out[None],
            grads_out[None],
            enter_total[None],
            leave_total[None],
            gain_total,
        )

    return jax.shard_map(
        local,
        mesh=mesh,
        in_specs=(
            P("section", None, None),
            P("section", None, None),
            P(),
            P(),
            P("section", None, None, None),
            P("section", None),
            P("section", None, "mp"),
            P("section", "mp", None),
            P("section", None),
        ),
        out_specs=(
            P("section", None, None),
            P("section", None, None),
            P("section", None, "mp"),
            P("section", "mp", None),
            P("section", None),
        ),
        check_vma=False,
    )
```
